32 devices in a mesh: row: 4 (over y, x), col: 8 (over z, core).
Axes of the slice: x: 2, y: 2, z: 4, core: 2. Of those that a mesh axis runs over, the one named last changes fastest.
Arguments:
- covariance: float32 [16384, 16384], P('row', 'col'), may hold values from -1 to 560
- seed_index: int32 [128], replicated, may hold values from 0 to 16383, as said below
Outputs:
- basis: float32 [16384, 384], P('row')
- projection: float32 [384, 256], replicated
- first_pass: float32 [384, 256], replicated
The draws below stay inside these ranges and needn't reach their ends.
Inputs may be any that keep to these rules, and one draw needn't show every extreme that they name: `seed_index`: 128 distinct column indices.
All inputs are finite; a program needn't handle non-finite values.
Results may differ from the reference program's by a relative error of at most 0.00019.
Values sent between devices are 32-bit elements; how exact they have to be, the bound alone decides.
A program may use at most 128 MiB of HBM per device.

```python
import jax
import jax.numpy as jnp
from jax import lax

N = 16384
B = 128
ITERS = 2


def draw_covariance(key, part):
    first_key = jax.random.fold_in(key, 11)
    second_key = jax.random.fold_in(key, 12)
    place = jnp.arange(N, dtype=jnp.float32) / jnp.float32(N - 1)
    noise = jax.random.normal(first_key, (N, N), jnp.float32)
    loading = jnp.exp(jax.random.uniform(second_key, (N,), jnp.float32, jnp.log(8.0), jnp.log(40.0)))
    loading = loading * (1.0 + 2.0 * place)
    symmetric = (noise + noise.T) * (3.0 / (2.0 * N) ** 0.5)
    return symmetric + jnp.diag(loading)


def draw_seed_index(key, part):
    order = jax.random.permutation(jax.random.fold_in(key, 21), N)
    return order[:B].astype(jnp.int32)


def setup_inputs(seed: int = 0) -> dict:
    arg_keys = jax.random.split(jax.random.key(seed), 3)
    covariance = draw_covariance(jax.random.fold_in(arg_keys[2], 71), 0)
    seed_index = draw_seed_index(jax.random.fold_in(arg_keys[2], 71), 0)
    return dict(covariance=covariance, seed_index=seed_index)


def product(left, right):
    return jnp.dot(left.astype(jnp.float32), right.astype(jnp.float32), precision=lax.Precision.HIGHEST, preferred_element_type=jnp.float32)

def orthonormal(block):
    gram = product(block.T, block)
    lower = jnp.linalg.cholesky(gram)
    basis_block = jax.scipy.linalg.solve_triangular(lower, block.T, lower=True).T
    return (basis_block, lower.T)

def reference(covariance, seed_index):
    start = jnp.take(covariance, seed_index.astype(jnp.int32), axis=1)
    current, upper = orthonormal(start)
    blocks = [current]
    projection = jnp.zeros(((ITERS + 1) * B, ITERS * B), jnp.float32)
    first_pass = jnp.zeros(((ITERS + 1) * B, ITERS * B), jnp.float32)
    for section in range(ITERS):
        image = product(covariance, current)
        stacked = jnp.concatenate(blocks, axis=1)
        first = product(stacked.T, image)
        once = image - product(stacked, first)
        second = product(stacked.T, once)
        twice = once - product(stacked, second)
        current, upper = orthonormal(twice)
        projection = projection.at[:(section + 1) * B, section * B:(section + 1) * B].set(first + second)
        projection = projection.at[(section + 1) * B:(section + 2) * B, section * B:(section + 1) * B].set(upper)
        first_pass = first_pass.at[:(section + 1) * B, section * B:(section + 1) * B].set(first)
        blocks.append(current)
    basis = jnp.concatenate(blocks, axis=1) * jnp.float32(N ** 0.5)
    return (basis, projection, first_pass)
```

```python
import jax
import jax.numpy as jnp
from jax import lax
from jax.sharding import PartitionSpec as P

N = 16384
ITERS = 2


def product(left, right):
    return jnp.dot(left, right, precision=lax.Precision.HIGH, preferred_element_type=jnp.float32)


def small_sum(value, axis):
    return jnp.sum(lax.all_gather(value, axis, axis=0), axis=0)


def finish_block(block, gram):
    lower = jnp.linalg.cholesky(gram)
    basis_block = jax.scipy.linalg.solve_triangular(lower, block.T, lower=True).T
    return (basis_block, lower.T)


def to_row_layout(piece, rows, cols):
    perm = [(r * cols + c, c * rows + r) for r in range(rows) for c in range(cols)]
    moved = lax.ppermute(piece, ("row", "col"), perm)
    return lax.all_gather(moved, "col", axis=0, tiled=True)


def solve(rows, cols, covariance, seed_index):
    row_count, col_count = covariance.shape
    width = seed_index.shape[0]
    row_place = lax.axis_index("row")
    piece_count = col_count // rows
    offsets = seed_index - row_place * row_count
    inside = (offsets >= 0) & (offsets < row_count)
    picked = jnp.take(covariance, jnp.clip(offsets, 0, row_count - 1), axis=0)
    start = lax.psum(jnp.where(inside[:, None], picked, 0.0), "row").T
    gram = small_sum(product(start.T, start), "col")
    vector, upper = finish_block(start, gram)
    piece = lax.dynamic_slice_in_dim(vector, row_place * piece_count, piece_count, 0)
    current = to_row_layout(piece, rows, cols)
    blocks = [current]
    projection = jnp.zeros(((ITERS + 1) * width, ITERS * width), jnp.float32)
    first_pass = jnp.zeros(((ITERS + 1) * width, ITERS * width), jnp.float32)
    for section in range(ITERS):
        stacked = jnp.concatenate(blocks, axis=1)
        if section == 0:
            image = lax.psum(product(covariance, vector), "col")
        else:
            partial_value = product(current.T, covariance).T
            piece = lax.psum_scatter(partial_value, "row", scatter_dimension=0, tiled=True)
            image = to_row_layout(piece, rows, cols)
        first = small_sum(product(stacked.T, image), "row")
        once = image - product(stacked, first)
        both = product(jnp.concatenate([stacked, once], axis=1).T, once)
        both = small_sum(both, "row")
        second, raw_gram = both[: (section + 1) * width], both[(section + 1) * width :]
        twice = once - product(stacked, second)
        gram = raw_gram - product(second.T, second)
        current, upper = finish_block(twice, gram)
        projection = projection.at[
            : (section + 1) * width, section * width : (section + 1) * width
        ].set(first + second)
        projection = projection.at[
            (section + 1) * width : (section + 2) * width, section * width : (section + 1) * width
        ].set(upper)
        first_pass = first_pass.at[
            : (section + 1) * width, section * width : (section + 1) * width
        ].set(first)
        blocks.append(current)
    basis = jnp.concatenate(blocks, axis=1) * jnp.float32(N**0.5)
    return (basis, projection, first_pass)


def solution(mesh):
    rows, cols = mesh.shape["row"], mesh.shape["col"]
    return jax.shard_map(
        lambda covariance, seed_index: solve(rows, cols, covariance, seed_index),
        mesh=mesh,
        in_specs=(P("row", "col"), P()),
        out_specs=(P("row", None), P(), P()),
        check_vma=False,
    )
```
